128 devices in a mesh: seq: 16 (over x_hi, z, core), tp: 8 (over y, x_lo).
Axes of the slice: x: 4 (x_hi: 2, x_lo: 2; x = x_hi * 2 + x_lo), y: 4, z: 4, core: 2. Of those that a mesh axis runs over, the one named last changes fastest.
Arguments:
- tokens: bfloat16 [2048, 8192], P('seq'), may hold values from -6 to 6
- conv_weight: float32 [4, 8192], replicated, may hold values from -3 to 3
- norm_gain: float32 [8192], replicated, may hold values from 0.25 to 1.75
- gate_weight: bfloat16 [8192, 14336], P('seq', 'tp'), may hold values from -0.0625 to 0.0625
- up_weight: bfloat16 [8192, 14336], P('seq', 'tp'), may hold values from -0.0625 to 0.0625
- down_weight: bfloat16 [14336, 8192], P('tp', 'seq'), may hold values from -0.046875 to 0.046875
Outputs:
- mixed_out: bfloat16 [2048, 8192], P(('seq', 'tp'))
The draws below stay inside these ranges and needn't reach their ends.
All inputs are finite; a program needn't handle non-finite values.
Results may differ from the reference program's by a relative error of at most 0.03.
Values may be sent and summed in bfloat16 or wider, within the bound.
No kernel may reach another device: no remote copies, remote signals or barrier semaphores. Data moves between devices by JAX's collectives and lax.ppermute only.
A program may use at most 64 MiB of HBM per device.

```python
import jax
import jax.numpy as jnp
from jax import lax

D = 8192
FF = 14336
TAPS = 4
TOKENS = 2048
N_SEQ = 16


def levels(key, dims, cuts, low, largest):
    def one(axis_at, parts):
        steps = jax.random.uniform(jax.random.fold_in(jax.random.fold_in(key, 6), axis_at), (parts,), jnp.float32, low / len(cuts), largest / len(cuts))
        return jnp.repeat(jnp.exp(steps), dims[axis_at] // parts).reshape((-1,) + (1,) * (len(dims) - axis_at - 1))

    loudness = one(*cuts[0])
    for cut in cuts[1:]:
        loudness = loudness * one(*cut)
    return loudness


def scatter_about(key, dims, deviation, limit, split=(), dtype=jnp.bfloat16):
    array = deviation * jax.random.normal(key, dims, jnp.float32)
    if split:
        array = array * levels(key, dims, split, -0.22, 0.18)
    return jnp.clip(array, -limit, limit).astype(dtype)


def setup_inputs(seed: int = 0) -> dict:
    keys = jax.random.split(jax.random.key(seed), 7)
    return {
        "tokens": scatter_about(keys[0], (TOKENS, D), 1.0, 6.0, ((0, 16),)),
        "conv_weight": scatter_about(keys[1], (TAPS, D), 0.5, 3.0, (), jnp.float32),
        "norm_gain": jnp.clip(1.0 + 0.15 * jax.random.normal(keys[2], (D,), jnp.float32), 0.25, 1.75),
        "gate_weight": scatter_about(keys[3], (D, FF), D ** -0.5, 0.0625, ((0, 16), (1, 8))),
        "up_weight": scatter_about(keys[4], (D, FF), D ** -0.5, 0.0625, ((0, 16), (1, 8))),
        "down_weight": scatter_about(keys[5], (FF, D), FF ** -0.5, 0.046875, ((0, 8), (1, 16))),
    }


def reference(tokens, conv_weight, norm_gain, gate_weight, up_weight, down_weight):
    inputs = tokens.astype(jnp.float32)
    tok_count = inputs.shape[0]
    model_width = inputs.shape[1]
    taps_count = conv_weight.shape[0]
    padded = jnp.concatenate([jnp.zeros((taps_count - 1, model_width), jnp.float32), inputs], 0)
    conv_out = jnp.zeros((tok_count, model_width), jnp.float32)
    for tap_index in range(taps_count):
        begin = taps_count - 1 - tap_index
        conv_out = conv_out + conv_weight[tap_index][None, :] * padded[begin:begin + tok_count]
    scale_rms = lax.rsqrt(lax.optimization_barrier(jnp.mean(conv_out * conv_out, axis=-1, keepdims=True)) + 1e-05)
    normed = (conv_out * scale_rms * norm_gain[None, :]).astype(jnp.bfloat16)
    group_width = model_width // N_SEQ
    hidden_width = gate_weight.shape[1]
    gate = jnp.zeros((tok_count, hidden_width), jnp.float32)
    up_sum = jnp.zeros((tok_count, hidden_width), jnp.float32)
    for group_index in range(N_SEQ):
        lower = group_index * group_width
        feats = normed[:, lower:lower + group_width]
        gate_part = jnp.dot(feats, gate_weight[lower:lower + group_width], preferred_element_type=jnp.float32)
        up_part = jnp.dot(feats, up_weight[lower:lower + group_width], preferred_element_type=jnp.float32)
        gate = gate + lax.optimization_barrier(gate_part.astype(jnp.bfloat16)).astype(jnp.float32)
        up_sum = up_sum + lax.optimization_barrier(up_part.astype(jnp.bfloat16)).astype(jnp.float32)
    hidden = (jax.nn.silu(gate) * up_sum).astype(jnp.bfloat16)
    return jnp.dot(hidden, down_weight, preferred_element_type=jnp.float32).astype(jnp.bfloat16)
```

```python
import jax
import jax.numpy as jnp
import numpy as np
from jax import lax
from jax.experimental import pallas as pl
from jax.experimental.pallas import tpu as pltpu
from jax.sharding import Mesh, PartitionSpec as P

CHIPS = ("xh", "z")
TP = ("y", "xl")
SEQ = ("xh", "z", "c")
BF16, F32 = jnp.bfloat16, jnp.float32


def conv_norm(tokens, edge, conv_weight, gain, peers):
    rows, width = tokens.shape
    taps = conv_weight.shape[0]
    group = width // peers
    step = 16
    lanes = 512
    pad = edge.shape[0]

    def body(tok, edg, cw, gn, out, ext, conv):
        i = pl.program_id(0)

        @pl.when(i == 0)
        def _():
            ext[:pad] = edg[...].astype(F32)

        @pl.when(i > 0)
        def _():
            ext[:pad] = ext[step : step + pad]

        ext[pad:] = tok[...].astype(F32)
        squares = jnp.zeros((step, 128), F32)
        for p in range(width // lanes):
            at = slice(p * lanes, (p + 1) * lanes)
            acc = cw[0:1, at] * ext[pad : pad + step, at]
            for k in range(1, taps):
                acc = acc + cw[k : k + 1, at] * ext[pad - k : pad - k + step, at]
            conv[:, at] = acc
            for j in range(lanes // 128):
                piece = acc[:, j * 128 : (j + 1) * 128]
                squares = squares + piece * piece
        mean = jnp.sum(squares, axis=1, keepdims=True) * (1.0 / width)
        scale = lax.rsqrt(mean + 1e-05)
        for p in range(width // lanes):
            at = slice(p * lanes, (p + 1) * lanes)
            lo = p * lanes % group
            out[p * lanes // group, :, lo : lo + lanes] = (conv[:, at] * scale * gn[:, at]).astype(BF16)

    return pl.pallas_call(
        body,
        grid=(rows // step,),
        in_specs=[
            pl.BlockSpec((step, width), lambda i: (i, 0)),
            pl.BlockSpec((pad, width), lambda i: (0, 0)),
            pl.BlockSpec((taps, width), lambda i: (0, 0)),
            pl.BlockSpec((1, width), lambda i: (0, 0)),
        ],
        out_specs=pl.BlockSpec((peers, step, group), lambda i: (0, i, 0)),
        out_shape=jax.ShapeDtypeStruct((peers, rows, group), BF16),
        scratch_shapes=[pltpu.VMEM((pad + step, width), F32), pltpu.VMEM((step, width), F32)],
        compiler_params=pltpu.CompilerParams(dimension_semantics=("arbitrary",)),
        name="conv_norm",
    )(tokens, edge, conv_weight, gain)


def gate_up(core, x, own_gate, other_gate, own_up, other_up, blocks):
    rows, depth = x.shape
    half, cols = own_gate.shape
    per = rows // blocks
    tile = 256

    def body(core_ref, x_ref, g0, g1, u0, u1, out):
        c = core_ref[0]
        mine = x_ref[:, pl.ds(pl.multiple_of(c * half, half), half)]
        theirs = x_ref[:, pl.ds(pl.multiple_of((1 - c) * half, half), half)]
        for k, (a, b) in enumerate(((g0, g1), (u0, u1))):
            total = jnp.dot(mine, a[...], preferred_element_type=F32) + jnp.dot(
                theirs, b[...], preferred_element_type=F32
            )
            out[:, k] = total.astype(BF16).reshape(blocks, per, tile)

    weight = pl.BlockSpec((half, tile), lambda n, c: (0, n))
    return pl.pallas_call(
        body,
        grid_spec=pltpu.PrefetchScalarGridSpec(
            num_scalar_prefetch=1,
            grid=(cols // tile,),
            in_specs=[pl.BlockSpec((rows, depth), lambda n, c: (0, 0))] + [weight] * 4,
            out_specs=pl.BlockSpec((blocks, 2, per, tile), lambda n, c: (0, 0, 0, n)),
        ),
        out_shape=jax.ShapeDtypeStruct((blocks, 2, per, cols), BF16),
        compiler_params=pltpu.CompilerParams(dimension_semantics=("arbitrary",)),
        name="gate_up",
    )(core, x, own_gate, other_gate, own_up, other_up)


def down(core, hidden, own, other, blocks, parts):
    rows, depth = hidden.shape
    half = own.shape[1]
    per = rows // blocks
    sub = per // parts

    def body(core_ref, h, d0, d1, out):
        c = core_ref[0]
        for at, w in ((c, d0), (1 - c, d1)):
            total = jnp.dot(h[...], w[...], preferred_element_type=F32).astype(BF16)
            out[:, 0, :, pl.ds(pl.multiple_of(at * half, half), half)] = total.reshape(parts, sub, half)

    return pl.pallas_call(
        body,
        grid_spec=pltpu.PrefetchScalarGridSpec(
            num_scalar_prefetch=1,
            grid=(blocks,),
            in_specs=[
                pl.BlockSpec((per, depth), lambda b, c: (b, 0)),
                pl.BlockSpec((depth, half), lambda b, c: (0, 0)),
                pl.BlockSpec((depth, half), lambda b, c: (0, 0)),
            ],
            out_specs=pl.BlockSpec((parts, 1, sub, 2 * half), lambda b, c: (0, b, 0, 0)),
        ),
        out_shape=jax.ShapeDtypeStruct((parts, blocks, sub, 2 * half), BF16),
        compiler_params=pltpu.CompilerParams(dimension_semantics=("arbitrary",)),
        name="down",
    )(core, hidden, own, other)


def shards(tokens, conv_weight, norm_gain, gate_weight, up_weight, down_weight):
    chips = lax.axis_size(CHIPS)
    parts = lax.axis_size(TP)
    seq = lax.axis_size(SEQ)
    core = lax.axis_index("c").astype(jnp.int32).reshape(1)
    swap = lambda w: lax.ppermute(w, "c", [(0, 1), (1, 0)])
    edge = lax.ppermute(tokens[-8:], SEQ, [(i, i + 1) for i in range(seq - 1)])
    gate_other, up_other, down_other = swap(gate_weight), swap(up_weight), swap(down_weight)
    normed = conv_norm(tokens, edge, conv_weight, norm_gain[None, :], chips)
    rows = lax.all_to_all(normed, CHIPS, split_axis=0, concat_axis=0, tiled=True)
    rows = rows.reshape(-1, rows.shape[2])
    sums = gate_up(core, rows, gate_weight, gate_other, up_weight, up_other, chips)
    mine = lax.psum_scatter(sums, CHIPS, scatter_dimension=0, tiled=True)[0].astype(F32)
    hidden = (jax.nn.silu(mine[0]) * mine[1]).astype(BF16)
    everyone = lax.all_gather(hidden, CHIPS, axis=0, tiled=True)
    terms = down(core, everyone, down_weight, down_other, chips, parts)
    arrived = lax.all_to_all(terms, TP, split_axis=0, concat_axis=0, tiled=True)
    summed = arrived.astype(F32).sum(axis=0).astype(BF16)
    out = lax.all_to_all(summed, CHIPS, split_axis=0, concat_axis=0, tiled=True)
    return jnp.transpose(out, (1, 0, 2)).reshape(out.shape[1], -1)


def solution(mesh):
    fine = Mesh(np.asarray(mesh.devices).reshape(2, 4, 2, 4, 2), ("xh", "z", "c", "y", "xl"))
    in_specs = (P(SEQ, None), P(), P(), P(SEQ, TP), P(SEQ, TP), P(TP, SEQ))
    out_specs = P(SEQ + TP, None)
    return jax.shard_map(shards, mesh=fine, in_specs=in_specs, out_specs=out_specs, check_vma=False)
```

```python
import jax
import jax.numpy as jnp
import numpy as np
from jax import lax
from jax.experimental import pallas as pl
from jax.experimental.pallas import tpu as pltpu
from jax.sharding import Mesh, PartitionSpec as P


CHIPS = ("xh", "z")
TP = ("y", "xl")
SEQ = ("xh", "z", "c")
SHAPE = {"xh": 2, "z": 4, "c": 2, "y": 4, "xl": 2}
STEPS = (0, 1, 3, 2)
PEERS = ((1, 0), (0, 3), (1, 3), (0, 1), (1, 1), (0, 2), (1, 2))
BF16, F32 = jnp.bfloat16, jnp.float32


def hop(x, dx, dz):
    pairs = []
    for a in range(SHAPE["xh"]):
        for b in range(SHAPE["z"]):
            pairs.append((a * 4 + b, (a + dx) % 2 * 4 + (b + dz) % 4))
    return lax.ppermute(x, CHIPS, pairs)


def conv_norm(place, tokens, edge, conv_weight, gain):
    rows, width = tokens.shape
    taps = conv_weight.shape[0]
    peers = 8
    group = width // peers
    step = 16
    lanes = 512
    pad = edge.shape[0]

    def body(at_ref, tok, edg, cw, gn, *rest):
        outs, (ext, conv) = rest[:peers], rest[peers:]
        i = pl.program_id(0)

        @pl.when(i == 0)
        def _():
            ext[:pad] = edg[...].astype(F32)

        @pl.when(i > 0)
        def _():
            ext[:pad] = ext[step : step + pad]

        ext[pad:] = tok[...].astype(F32)
        squares = jnp.zeros((step, 128), F32)
        for p in range(width // lanes):
            at = slice(p * lanes, (p + 1) * lanes)
            acc = cw[0:1, at] * ext[pad : pad + step, at]
            for k in range(1, taps):
                acc = acc + cw[k : k + 1, at] * ext[pad - k : pad - k + step, at]
            conv[:, at] = acc
            for j in range(lanes // 128):
                piece = acc[:, j * 128 : (j + 1) * 128]
                squares = squares + piece * piece
        mean = jnp.sum(squares, axis=1, keepdims=True) * (1.0 / width)
        scale = lax.rsqrt(mean + 1e-05)
        for p in range(peers):
            dx, dz = p // 4, p % 4
            peer = (at_ref[1] + dx) % 2 * 4 + (at_ref[2] + dz) % 4
            at = pl.ds(pl.multiple_of(peer * group, group), group)
            outs[p][...] = (conv[:, at] * scale * gn[:, at]).astype(BF16)

    return pl.pallas_call(
        body,
        grid_spec=pltpu.PrefetchScalarGridSpec(
            num_scalar_prefetch=1,
            grid=(rows // step,),
            in_specs=[
                pl.BlockSpec((step, width), lambda i, s: (i, 0)),
                pl.BlockSpec((pad, width), lambda i, s: (0, 0)),
                pl.BlockSpec((taps, width), lambda i, s: (0, 0)),
                pl.BlockSpec((1, width), lambda i, s: (0, 0)),
            ],
            out_specs=[pl.BlockSpec((step, group), lambda i, s: (i, 0))] * peers,
            scratch_shapes=[pltpu.VMEM((pad + step, width), F32), pltpu.VMEM((step, width), F32)],
        ),
        out_shape=[jax.ShapeDtypeStruct((rows, group), BF16)] * peers,
        compiler_params=pltpu.CompilerParams(dimension_semantics=("arbitrary",), vmem_limit_bytes=12 * 2**20),
        cost_estimate=pl.CostEstimate(flops=4000000000, bytes_accessed=4 * rows * width, transcendentals=0),
        name="conv_norm",
    )(place, tokens, edge, conv_weight, gain)


def gate_up(place, near, far, own_gate, other_gate, own_up, other_up):
    per, depth = near.shape
    half, cols = own_gate.shape
    tile = 256
    first = 3

    def body(at_ref, near_ref, far_ref, g0, g1, u0, u1, one, two_near, two_far):
        c = at_ref[0]
        mine = pl.ds(pl.multiple_of(c * half, half), half)
        theirs = pl.ds(pl.multiple_of((1 - c) * half, half), half)

        def product(n, own, other):
            at = pl.ds(pl.multiple_of(n * tile, tile), tile)
            x_mine = jnp.concatenate([near_ref[:, mine], far_ref[:, mine]], 0)
            x_theirs = jnp.concatenate([near_ref[:, theirs], far_ref[:, theirs]], 0)
            total = jnp.dot(x_mine, own[:, at], preferred_element_type=F32) + jnp.dot(
                x_theirs, other[:, at], preferred_element_type=F32
            )
            return total.astype(BF16)

        def to_one(n, _):
            at = pl.ds(pl.multiple_of(n * tile, tile), tile)
            for k, (a, b) in enumerate(((g0, g1), (u0, u1))):
                total = product(n, a, b)
                one[0, k, :, at] = total[:per]
                one[1, k, :, at] = total[per:]
            return 0

        def to_two(n, _):
            at = pl.ds(pl.multiple_of(n * tile, tile), tile)
            for k, (a, b) in enumerate(((g0, g1), (u0, u1))):
                total = product(n + first, a, b)
                two_near[k, :, at] = total[:per]
                two_far[k, :, at] = total[per:]
            return 0

        lax.fori_loop(0, first, to_one, 0)
        lax.fori_loop(0, cols // tile - first, to_two, 0)

    vmem = pl.BlockSpec(memory_space=pltpu.VMEM)
    two_shape = jax.ShapeDtypeStruct((2, per, cols - first * tile), BF16)
    return pl.pallas_call(
        body,
        in_specs=[pl.BlockSpec(memory_space=pltpu.SMEM)] + [vmem] * 6,
        out_specs=[vmem] * 3,
        out_shape=[jax.ShapeDtypeStruct((2, 2, per, first * tile), BF16), two_shape, two_shape],
        compiler_params=pltpu.CompilerParams(vmem_limit_bytes=24 * 2**20),
        cost_estimate=pl.CostEstimate(
            flops=8 * per * depth * cols, bytes_accessed=8 * half * cols, transcendentals=0
        ),
        name="gate_up",
    )(place, near, far, own_gate, other_gate, own_up, other_up)


def down(place, step, near, far, own, other, parts, terms):
    per, depth = near.shape
    half = own.shape[1]
    sub = per // parts

    def body(at_ref, h0, h1, d0, d1, *rest):
        out = rest[-1]
        c = at_ref[0]
        g = pl.program_id(0)

        def write(h):
            for at, w in ((c, d0), (1 - c, d1)):
                total = jnp.dot(h[...], w[...], preferred_element_type=F32).astype(BF16)
                out[:, 0, :, pl.ds(pl.multiple_of(at * half, half), half)] = total.reshape(parts, sub, half)

        @pl.when(g == 0)
        def _():
            write(h0)

        @pl.when(g == 1)
        def _():
            write(h1)

    def block(g, s):
        return (0, (s[1] + g) % 2 * 4 + (s[2] + step) % 4, 0, 0)

    rows = weight = pl.BlockSpec(memory_space=pltpu.VMEM)
    carried = [] if terms is None else [terms]
    return pl.pallas_call(
        body,
        grid_spec=pltpu.PrefetchScalarGridSpec(
            num_scalar_prefetch=1,
            grid=(2,),
            in_specs=[rows, rows, weight, weight] + [pl.BlockSpec(memory_space=pl.ANY)] * len(carried),
            out_specs=pl.BlockSpec((parts, 1, sub, 2 * half), block),
        ),
        out_shape=jax.ShapeDtypeStruct((parts, 8, sub, 2 * half), BF16),
        input_output_aliases={5: 0} if carried else {},
        compiler_params=pltpu.CompilerParams(dimension_semantics=("arbitrary",), vmem_limit_bytes=12 * 2**20),
        cost_estimate=pl.CostEstimate(flops=8 * per * depth * half, bytes_accessed=4 * depth * half, transcendentals=0),
        name="down",
    )(place, near, far, own, other, *carried)


def total(*terms):
    out = terms[0].astype(F32)
    for t in terms[1:]:
        out = out + t.astype(F32)
    return out


def swiglu(both):
    return (jax.nn.silu(both[0]) * both[1]).astype(BF16)


def shards(tokens, conv_weight, norm_gain, gate_weight, up_weight, down_weight):
    parts = lax.axis_size(TP)
    seq = lax.axis_size(SEQ)
    place = jnp.stack([lax.axis_index(a).astype(jnp.int32) for a in ("c", "xh", "z")])
    swap = lambda w: lax.ppermute(w, "c", [(0, 1), (1, 0)])
    edge = lax.ppermute(tokens[-8:], SEQ, [(i, i + 1) for i in range(seq - 1)])
    gate_other = swap(gate_weight)
    up_other = swap(up_weight)
    down_other = swap(down_weight)
    normed = conv_norm(place, tokens, edge, conv_weight, norm_gain[None, :])
    rows = {(0, 0): normed[0]}
    for dx, dz in PEERS:
        rows[dx, -dz % 4] = hop(normed[dx * 4 + dz], dx, dz)
    one, near, far, one_in, far_in = {}, {}, {}, {}, {}
    for e in STEPS:
        one[e], near[e], far[e] = gate_up(place, rows[0, e], rows[1, e], gate_weight, gate_other, up_weight, up_other)
        far_in[e] = hop(far[e], 1, 0)
        if e:
            one_in[e] = hop(one[e], 0, e)
    two_in = {}
    for e in STEPS[1:]:
        both = total(near[e], far_in[e]).astype(BF16)
        two_in[e] = hop(both, 0, e)
    firsts = [one[0]] + [one_in[e] for e in STEPS[1:]]
    across = total(*[f[1] for f in firsts]).astype(BF16)
    last = hop(across, 1, 0)
    left = total(*[f[0] for f in firsts], last)
    right = total(near[0], far_in[0], *[two_in[e] for e in STEPS[1:]])
    hidden = jnp.concatenate([swiglu(left), swiglu(right)], 1)
    blocks = {(0, 0): hidden}
    for dx, dz in PEERS:
        blocks[dx, -dz % 4] = hop(hidden, dx, dz)
    terms = None
    for e in STEPS:
        terms = down(place, e, blocks[0, e], blocks[1, e], down_weight, down_other, parts, terms)
    arrived = lax.all_to_all(terms, TP, split_axis=0, concat_axis=0, tiled=True)
    summed = arrived.astype(F32).sum(axis=0).astype(BF16)
    out = lax.all_to_all(summed, CHIPS, split_axis=0, concat_axis=0, tiled=True)
    return jnp.transpose(out, (1, 0, 2)).reshape(out.shape[1], -1)


def solution(mesh):
    fine = Mesh(np.asarray(mesh.devices).reshape(*SHAPE.values()), tuple(SHAPE))
    in_specs = (P(SEQ, None), P(), P(), P(SEQ, TP), P(SEQ, TP), P(TP, SEQ))
    out_specs = P(SEQ + TP, None)
    return jax.shard_map(shards, mesh=fine, in_specs=in_specs, out_specs=out_specs, check_vma=False)
```

```python
import jax
import jax.numpy as jnp
import numpy as np
from jax import lax
from jax.experimental import pallas as pl
from jax.experimental.pallas import tpu as pltpu
from jax.sharding import Mesh, PartitionSpec as P


CHIPS = ("xh", "z")
TP = ("y", "xl")
SEQ = ("xh", "z", "c")
SHAPE = {"xh": 2, "z": 4, "c": 2, "y": 4, "xl": 2}
STEPS = (1, 3, 2, 0)
PEERS = ((0, 3), (1, 3), (0, 1), (1, 1), (0, 2), (1, 2), (1, 0))
BF16, F32 = jnp.bfloat16, jnp.float32


def hop(x, dx, dz):
    pairs = []
    for a in range(SHAPE["xh"]):
        for b in range(SHAPE["z"]):
            pairs.append((a * 4 + b, (a + dx) % 2 * 4 + (b + dz) % 4))
    return lax.ppermute(x, CHIPS, pairs)


def conv_norm(place, tokens, edge, conv_weight, gain):
    rows, width = tokens.shape
    taps = conv_weight.shape[0]
    peers = 8
    group = width // peers
    step = 16
    lanes = 512
    pad = edge.shape[0]

    def body(at_ref, tok, edg, cw, gn, *rest):
        outs, (ext, conv) = rest[:peers], rest[peers:]
        i = pl.program_id(0)

        @pl.when(i == 0)
        def _():
            ext[:pad] = edg[...].astype(F32)

        @pl.when(i > 0)
        def _():
            ext[:pad] = ext[step : step + pad]

        ext[pad:] = tok[...].astype(F32)
        squares = jnp.zeros((step, 128), F32)
        for p in range(width // lanes):
            at = slice(p * lanes, (p + 1) * lanes)
            acc = cw[0:1, at] * ext[pad : pad + step, at]
            for k in range(1, taps):
                acc = acc + cw[k : k + 1, at] * ext[pad - k : pad - k + step, at]
            conv[:, at] = acc
            for j in range(lanes // 128):
                piece = acc[:, j * 128 : (j + 1) * 128]
                squares = squares + piece * piece
        mean = jnp.sum(squares, axis=1, keepdims=True) * (1.0 / width)
        scale = lax.rsqrt(mean + 1e-05)
        for p in range(peers):
            dx, dz = p // 4, p % 4
            peer = (at_ref[1] + dx) % 2 * 4 + (at_ref[2] + dz) % 4
            at = pl.ds(pl.multiple_of(peer * group, group), group)
            outs[p][...] = (conv[:, at] * scale * gn[:, at]).astype(BF16)

    return pl.pallas_call(
        body,
        grid_spec=pltpu.PrefetchScalarGridSpec(
            num_scalar_prefetch=1,
            grid=(rows // step,),
            in_specs=[
                pl.BlockSpec((step, width), lambda i, s: (i, 0)),
                pl.BlockSpec((pad, width), lambda i, s: (0, 0)),
                pl.BlockSpec((taps, width), lambda i, s: (0, 0)),
                pl.BlockSpec((1, width), lambda i, s: (0, 0)),
            ],
            out_specs=[pl.BlockSpec((step, group), lambda i, s: (i, 0))] * peers,
            scratch_shapes=[pltpu.VMEM((pad + step, width), F32), pltpu.VMEM((step, width), F32)],
        ),
        out_shape=[jax.ShapeDtypeStruct((rows, group), BF16)] * peers,
        compiler_params=pltpu.CompilerParams(dimension_semantics=("arbitrary",), vmem_limit_bytes=12 * 2**20),
        cost_estimate=pl.CostEstimate(flops=4000000000, bytes_accessed=4 * rows * width, transcendentals=0),
        name="conv_norm",
    )(place, tokens, edge, conv_weight, gain)


def gate_up(place, near, far, own_gate, other_gate, own_up, other_up):
    per, depth = near.shape
    half, cols = own_gate.shape
    tile = 256
    first = 3

    def body(at_ref, near_ref, far_ref, g0, g1, u0, u1, one, two_near, two_far):
        c = at_ref[0]
        mine = pl.ds(pl.multiple_of(c * half, half), half)
        theirs = pl.ds(pl.multiple_of((1 - c) * half, half), half)

        x_mine = jnp.concatenate([near_ref[:, mine], far_ref[:, mine]], 0)
        x_theirs = jnp.concatenate([near_ref[:, theirs], far_ref[:, theirs]], 0)

        def product(at, own, other):
            total = jnp.dot(x_mine, own[:, at], preferred_element_type=F32) + jnp.dot(
                x_theirs, other[:, at], preferred_element_type=F32
            )
            return total.astype(BF16)

        split = first * tile
        for k, (a, b) in enumerate(((g0, g1), (u0, u1))):
            for n in range(0, cols, tile):
                total = product(slice(n, n + tile), a, b)
                if n < split:
                    one[0, k, :, n : n + tile] = total[:per]
                    one[1, k, :, n : n + tile] = total[per:]
                else:
                    two_near[k, :, n - split : n - split + tile] = total[:per]
                    two_far[k, :, n - split : n - split + tile] = total[per:]

    vmem = pl.BlockSpec(memory_space=pltpu.VMEM)
    two_shape = jax.ShapeDtypeStruct((2, per, cols - first * tile), BF16)
    return pl.pallas_call(
        body,
        in_specs=[pl.BlockSpec(memory_space=pltpu.SMEM)] + [vmem] * 6,
        out_specs=[vmem] * 3,
        out_shape=[jax.ShapeDtypeStruct((2, 2, per, first * tile), BF16), two_shape, two_shape],
        compiler_params=pltpu.CompilerParams(vmem_limit_bytes=24 * 2**20),
        cost_estimate=pl.CostEstimate(
            flops=8 * per * depth * cols, bytes_accessed=8 * half * cols, transcendentals=0
        ),
        name="gate_up",
    )(place, near, far, own_gate, other_gate, own_up, other_up)


def down(place, step, left, right, own, other, parts, terms):
    per = right[0].shape[0]
    cut = left[0].shape[-1]
    depth, half = own.shape
    sub = per // parts
    pair = len(left) == 1

    def body(at_ref, *rest):
        lefts, (r0, r1, d0, d1) = rest[: len(left)], rest[len(left) : len(left) + 4]
        out = rest[-1]
        c = at_ref[0]
        g = pl.program_id(0)

        def write(l, r):
            for at, w in ((c, d0), (1 - c, d1)):
                total = jnp.dot(l, w[:cut], preferred_element_type=F32)
                total = total + jnp.dot(r, w[cut:], preferred_element_type=F32)
                out[:, 0, :, pl.ds(pl.multiple_of(at * half, half), half)] = total.astype(BF16).reshape(
                    parts, sub, half
                )

        @pl.when(g == 0)
        def _():
            write(lefts[0][0] if pair else lefts[0][...], r0[...])

        @pl.when(g == 1)
        def _():
            write(lefts[0][1] if pair else lefts[1][...], r1[...])

    def block(g, s):
        return (0, (s[1] + g) % 2 * 4 + (s[2] + step) % 4, 0, 0)

    whole = pl.BlockSpec(memory_space=pltpu.VMEM)
    carried = [] if terms is None else [terms]
    inputs = [*left, *right, own, other]
    return pl.pallas_call(
        body,
        grid_spec=pltpu.PrefetchScalarGridSpec(
            num_scalar_prefetch=1,
            grid=(2,),
            in_specs=[whole] * len(inputs) + [pl.BlockSpec(memory_space=pl.ANY)] * len(carried),
            out_specs=pl.BlockSpec((parts, 1, sub, 2 * half), block),
        ),
        out_shape=jax.ShapeDtypeStruct((parts, 8, sub, 2 * half), BF16),
        input_output_aliases={1 + len(inputs): 0} if carried else {},
        compiler_params=pltpu.CompilerParams(dimension_semantics=("arbitrary",), vmem_limit_bytes=12 * 2**20),
        cost_estimate=pl.CostEstimate(flops=8 * per * depth * half, bytes_accessed=4 * depth * half, transcendentals=0),
        name="down",
    )(place, *inputs, *carried)


def total(*terms):
    out = terms[0].astype(F32)
    for t in terms[1:]:
        out = out + t.astype(F32)
    return out


def swiglu(both):
    return (jax.nn.silu(both[0]) * both[1]).astype(BF16)


def shards(tokens, conv_weight, norm_gain, gate_weight, up_weight, down_weight):
    parts = lax.axis_size(TP)
    seq = lax.axis_size(SEQ)
    place = jnp.stack([lax.axis_index(a).astype(jnp.int32) for a in ("c", "xh", "z")])
    swap = lambda w: lax.ppermute(w, "c", [(0, 1), (1, 0)])
    edge = lax.ppermute(tokens[-8:], SEQ, [(i, i + 1) for i in range(seq - 1)])
    gate_other = swap(gate_weight)
    up_other = swap(up_weight)
    down_other = swap(down_weight)
    normed = conv_norm(place, tokens, edge, conv_weight, norm_gain[None, :])
    rows = {(0, 0): normed[0]}
    for dx, dz in PEERS:
        rows[dx, -dz % 4] = hop(normed[dx * 4 + dz], dx, dz)
    one, near, far, one_in, far_in = {}, {}, {}, {}, {}
    for e in STEPS:
        one[e], near[e], far[e] = gate_up(place, rows[0, e], rows[1, e], gate_weight, gate_other, up_weight, up_other)
        far_in[e] = hop(far[e], 1, 0)
        if e:
            one_in[e] = hop(one[e], 0, e)
    two_in = {}
    for e in STEPS[:3]:
        both = total(near[e], far_in[e]).astype(BF16)
        two_in[e] = hop(both, 0, e)
    firsts = [one[0]] + [one_in[e] for e in STEPS[:3]]
    across = total(*[f[1] for f in firsts]).astype(BF16)
    last = hop(across, 1, 0)
    left = swiglu(total(*[f[0] for f in firsts], last))
    left_far = hop(left, 1, 0)
    right = swiglu(total(near[0], far_in[0], *[two_in[e] for e in STEPS[:3]]))
    right_far = {0: hop(right, 1, 0)}
    right_near = {0: right}
    for e in STEPS[:3]:
        right_near[e] = hop(right, 0, -e % 4)
    pair = jnp.stack([left, left_far])
    lefts = {0: (left, left_far)}
    for e in STEPS[:3]:
        lefts[e] = (hop(pair, 0, -e % 4),)
    for e in STEPS[:3]:
        right_far[e] = hop(right_near[e], 1, 0)
    terms = None
    for e in (0, 1, 3, 2):
        rights = (right_near[e], right_far[e])
        terms = down(place, e, lefts[e], rights, down_weight, down_other, parts, terms)
    arrived = lax.all_to_all(terms, TP, split_axis=0, concat_axis=0, tiled=True)
    summed = arrived.astype(F32).sum(axis=0).astype(BF16)
    out = lax.all_to_all(summed, CHIPS, split_axis=0, concat_axis=0, tiled=True)
    return jnp.transpose(out, (1, 0, 2)).reshape(out.shape[1], -1)


def solution(mesh):
    fine = Mesh(np.asarray(mesh.devices).reshape(*SHAPE.values()), tuple(SHAPE))
    in_specs = (P(SEQ, None), P(), P(), P(SEQ, TP), P(SEQ, TP), P(TP, SEQ))
    out_specs = P(SEQ + TP, None)
    return jax.shard_map(shards, mesh=fine, in_specs=in_specs, out_specs=out_specs, check_vma=False)
```

```python
import jax
import jax.numpy as jnp
import numpy as np
from jax import lax
from jax.experimental import pallas as pl
from jax.experimental.pallas import tpu as pltpu
from jax.sharding import Mesh, PartitionSpec as P


CHIPS = ("xh", "z")
TP = ("y", "xl")
SEQ = ("xh", "z", "c")
SHAPE = {"xh": 2, "z": 4, "c": 2, "y": 4, "xl": 2}
STEPS = (1, 3, 2, 0)
PEERS = ((0, 3), (0, 1), (1, 3), (1, 1), (0, 2), (1, 2), (1, 0))
BF16, F32 = jnp.bfloat16, jnp.float32


def hop(x, dx, dz):
    pairs = []
    for a in range(SHAPE["xh"]):
        for b in range(SHAPE["z"]):
            pairs.append((a * 4 + b, (a + dx) % 2 * 4 + (b + dz) % 4))
    return lax.ppermute(x, CHIPS, pairs)


def conv_rows(ext, tok, cw, gn, conv, emit, place):
    step, width = tok.shape
    taps = cw.shape[0]
    lanes = 512
    pad = ext.shape[0] - step
    group = width // 8
    ext[pad:] = tok.astype(F32)
    squares = jnp.zeros((step, 128), F32)
    for p in range(width // lanes):
        at = slice(p * lanes, (p + 1) * lanes)
        acc = cw[0:1, at] * ext[pad : pad + step, at]
        for k in range(1, taps):
            acc = acc + cw[k : k + 1, at] * ext[pad - k : pad - k + step, at]
        conv[:, at] = acc
        for j in range(lanes // 128):
            piece = acc[:, j * 128 : (j + 1) * 128]
            squares = squares + piece * piece
    mean = jnp.sum(squares, axis=1, keepdims=True) * (1.0 / width)
    scale = lax.rsqrt(mean + 1e-05)
    for p in range(8):
        dx, dz = p // 4, p % 4
        peer = (place[1] + dx) % 2 * 4 + (place[2] + dz) % 4
        at = pl.ds(pl.multiple_of(peer * group, group), group)
        emit(p, (conv[:, at] * scale * gn[:, at]).astype(BF16))


STEP, PAD = 16, 8


def conv_main(place, tokens, conv_weight, gain):
    rows, width = tokens.shape
    tiles = rows // STEP

    def body(at_ref, tok_h, cw_h, gn_h, *rest):
        outs, (tok, cw, gn, ext, conv, sems) = rest[:8], rest[8:]
        weights = pltpu.make_async_copy(cw_h, cw, sems.at[tiles])
        gains = pltpu.make_async_copy(gn_h, gn, sems.at[tiles + 1])

        def load(i):
            at = pl.ds(pl.multiple_of(i * STEP, STEP), STEP)
            return pltpu.make_async_copy(tok_h.at[at], tok.at[at], sems.at[i])

        for i in range(2):
            load(i).start()
        weights.start()
        gains.start()
        for i in range(2, tiles):
            load(i).start()
        load(0).wait()
        ext[:PAD] = tok[:STEP].astype(F32)[STEP - PAD :]
        weights.wait()
        gains.wait()

        def tile(i, _):
            load(i).wait()
            at = pl.ds(pl.multiple_of(i * STEP, STEP), STEP)

            def emit(p, value):
                outs[p][at, :] = value

            conv_rows(ext, tok[at, :], cw, gn, conv, emit, at_ref)
            ext[:PAD] = ext[STEP : STEP + PAD]
            return 0

        lax.fori_loop(1, tiles, tile, 0)

    hbm = pl.BlockSpec(memory_space=pltpu.HBM)
    vmem = pl.BlockSpec(memory_space=pltpu.VMEM)
    block = jax.ShapeDtypeStruct((rows, width // 8), BF16)
    kept = [jax.ShapeDtypeStruct(a.shape, a.dtype) for a in (tokens, conv_weight, gain)]
    return pl.pallas_call(
        body,
        in_specs=[pl.BlockSpec(memory_space=pltpu.SMEM), hbm, hbm, hbm],
        out_specs=[vmem] * 11,
        out_shape=[block] * 8 + kept,
        scratch_shapes=[
            pltpu.VMEM((PAD + STEP, width), F32),
            pltpu.VMEM((STEP, width), F32),
            pltpu.SemaphoreType.DMA((tiles + 2,)),
        ],
        compiler_params=pltpu.CompilerParams(vmem_limit_bytes=16 * 2**20),
        cost_estimate=pl.CostEstimate(flops=4000000000, bytes_accessed=4 * rows * width, transcendentals=0),
        name="conv_main",
    )(place, *[pltpu.with_memory_space_constraint(a, pltpu.HBM) for a in (tokens, conv_weight, gain)])


def conv_head(place, edge, tokens, conv_weight, gain, blocks):
    width = tokens.shape[1]

    def body(at_ref, edg, tok, cw, gn, *rest):
        outs, (ext, conv, tile, sems) = rest[8:16], rest[16:]
        ext[:PAD] = edg[...].astype(F32)
        copies = []

        def emit(p, value):
            tile[p] = value
            copies.append(pltpu.make_async_copy(tile.at[p], outs[p].at[pl.ds(0, STEP)], sems.at[p]))
            copies[-1].start()

        conv_rows(ext, tok[:STEP, :], cw, gn, conv, emit, at_ref)
        for copy in copies:
            copy.wait()

    vmem = pl.BlockSpec(memory_space=pltpu.VMEM)
    anywhere = pl.BlockSpec(memory_space=pl.ANY)
    return pl.pallas_call(
        body,
        in_specs=[pl.BlockSpec(memory_space=pltpu.SMEM)] + [vmem] * 4 + [anywhere] * 8,
        out_specs=[anywhere] * 8,
        out_shape=[jax.ShapeDtypeStruct(b.shape, b.dtype) for b in blocks],
        input_output_aliases={5 + i: i for i in range(8)},
        scratch_shapes=[
            pltpu.VMEM((PAD + STEP, width), F32),
            pltpu.VMEM((STEP, width), F32),
            pltpu.VMEM((8, STEP, width // 8), BF16),
            pltpu.SemaphoreType.DMA((8,)),
        ],
        compiler_params=pltpu.CompilerParams(vmem_limit_bytes=16 * 2**20),
        cost_estimate=pl.CostEstimate(flops=400000000, bytes_accessed=4 * STEP * width, transcendentals=0),
        name="conv_head",
    )(place, edge, tokens, conv_weight, gain, *blocks)


CUT = 768


def gate_up(place, near, far, own_gate, other_gate, own_up, other_up, lo, hi, joined):
    per, depth = near.shape
    half = own_gate.shape[0]
    tile = 256

    def body(at_ref, near_ref, far_ref, g0, g1, u0, u1, *outs):
        c = at_ref[0]
        mine = pl.ds(pl.multiple_of(c * half, half), half)
        theirs = pl.ds(pl.multiple_of((1 - c) * half, half), half)
        x_mine = jnp.concatenate([near_ref[:, mine], far_ref[:, mine]], 0)
        x_theirs = jnp.concatenate([near_ref[:, theirs], far_ref[:, theirs]], 0)
        for k, (a, b) in enumerate(((g0, g1), (u0, u1))):
            for n in range(lo, hi, tile):
                at = slice(n, n + tile)
                total = jnp.dot(x_mine, a[:, at], preferred_element_type=F32) + jnp.dot(
                    x_theirs, b[:, at], preferred_element_type=F32
                )
                total = total.astype(BF16)
                to = slice(n - lo, n - lo + tile)
                if joined:
                    outs[0][0, k, :, to] = total[:per]
                    outs[0][1, k, :, to] = total[per:]
                else:
                    outs[0][k, :, to] = total[:per]
                    outs[1][k, :, to] = total[per:]

    vmem = pl.BlockSpec(memory_space=pltpu.VMEM)
    width = hi - lo
    if joined:
        shapes = [jax.ShapeDtypeStruct((2, 2, per, width), BF16)]
    else:
        shapes = [jax.ShapeDtypeStruct((2, per, width), BF16)] * 2
    return pl.pallas_call(
        body,
        in_specs=[pl.BlockSpec(memory_space=pltpu.SMEM)] + [vmem] * 6,
        out_specs=[vmem] * len(shapes),
        out_shape=shapes,
        compiler_params=pltpu.CompilerParams(vmem_limit_bytes=24 * 2**20),
        cost_estimate=pl.CostEstimate(
            flops=8 * per * depth * width, bytes_accessed=8 * half * width, transcendentals=0
        ),
        name="gate_up",
    )(place, near, far, own_gate, other_gate, own_up, other_up)


def down(place, step, left, right, own, other, parts, terms):
    per = right[0].shape[0]
    cut = left[0].shape[-1]
    depth, half = own.shape
    sub = per // parts
    pair = len(left) == 1

    def body(at_ref, *rest):
        lefts, (r0, r1, d0, d1) = rest[: len(left)], rest[len(left) : len(left) + 4]
        out = rest[-1]
        c = at_ref[0]
        g = pl.program_id(0)

        def write(l, r):
            for at, w in ((c, d0), (1 - c, d1)):
                total = jnp.dot(l, w[:cut], preferred_element_type=F32)
                total = total + jnp.dot(r, w[cut:], preferred_element_type=F32)
                out[:, 0, :, pl.ds(pl.multiple_of(at * half, half), half)] = total.astype(BF16).reshape(
                    parts, sub, half
                )

        @pl.when(g == 0)
        def _():
            write(lefts[0][0] if pair else lefts[0][...], r0[...])

        @pl.when(g == 1)
        def _():
            write(lefts[0][1] if pair else lefts[1][...], r1[...])

    def block(g, s):
        return (0, (s[1] + g) % 2 * 4 + (s[2] + step) % 4, 0, 0)

    whole = pl.BlockSpec(memory_space=pltpu.VMEM)
    carried = [] if terms is None else [terms]
    inputs = [*left, *right, own, other]
    return pl.pallas_call(
        body,
        grid_spec=pltpu.PrefetchScalarGridSpec(
            num_scalar_prefetch=1,
            grid=(2,),
            in_specs=[whole] * len(inputs) + [pl.BlockSpec(memory_space=pl.ANY)] * len(carried),
            out_specs=pl.BlockSpec((parts, 1, sub, 2 * half), block),
        ),
        out_shape=jax.ShapeDtypeStruct((parts, 8, sub, 2 * half), BF16),
        input_output_aliases={1 + len(inputs): 0} if carried else {},
        compiler_params=pltpu.CompilerParams(dimension_semantics=("arbitrary",), vmem_limit_bytes=12 * 2**20),
        cost_estimate=pl.CostEstimate(flops=8 * per * depth * half, bytes_accessed=4 * depth * half, transcendentals=0),
        name="down",
    )(place, *inputs, *carried)


def total(*terms):
    out = terms[0].astype(F32)
    for t in terms[1:]:
        out = out + t.astype(F32)
    return out


def swiglu(both):
    return (jax.nn.silu(both[0]) * both[1]).astype(BF16)


def shards(tokens, conv_weight, norm_gain, gate_weight, up_weight, down_weight):
    parts = lax.axis_size(TP)
    seq = lax.axis_size(SEQ)
    place = jnp.stack([lax.axis_index(a).astype(jnp.int32) for a in ("c", "xh", "z")])
    swap = lambda w: lax.ppermute(w, "c", [(0, 1), (1, 0)])
    edge = lax.ppermute(tokens[-8:], SEQ, [(i, i + 1) for i in range(seq - 1)])
    gate_other = swap(gate_weight)
    up_other = swap(up_weight)
    down_other = swap(down_weight)
    *normed, held, taps, gain = conv_main(place, tokens, conv_weight, norm_gain[None, :])
    normed = conv_head(place, edge, held, taps, gain, normed)
    rows = {(0, 0): normed[0]}
    for dx, dz in PEERS:
        rows[dx, -dz % 4] = hop(normed[dx * 4 + dz], dx, dz)
    one, near, far, one_in, far_in = {}, {}, {}, {}, {}
    weights = (gate_weight, gate_other, up_weight, up_other)
    cols = gate_weight.shape[1]
    for e in STEPS:
        (one[e],) = gate_up(place, rows[0, e], rows[1, e], *weights, 0, CUT, True)
        if e:
            one_in[e] = hop(one[e], 0, e)
        near[e], far[e] = gate_up(place, rows[0, e], rows[1, e], *weights, CUT, cols, False)
        far_in[e] = hop(far[e], 1, 0)
    two_in = {}
    for e in STEPS[:3]:
        both = total(near[e], far_in[e]).astype(BF16)
        two_in[e] = hop(both, 0, e)
    firsts = [one[0]] + [one_in[e] for e in STEPS[:3]]
    across = total(*[f[1] for f in firsts]).astype(BF16)
    last = hop(across, 1, 0)
    left = swiglu(total(*[f[0] for f in firsts], last))
    left_far = hop(left, 1, 0)
    right = swiglu(total(near[0], far_in[0], *[two_in[e] for e in STEPS[:3]]))
    right_far = {0: hop(right, 1, 0)}
    right_near = {0: right}
    for e in STEPS[:3]:
        right_near[e] = hop(right, 0, -e % 4)
    pair = jnp.stack([left, left_far])
    lefts = {0: (left, left_far)}
    for e in STEPS[:3]:
        lefts[e] = (hop(pair, 0, -e % 4),)
    for e in STEPS[:3]:
        right_far[e] = hop(right_near[e], 1, 0)
    terms = None
    for e in (0, 1, 3, 2):
        rights = (right_near[e], right_far[e])
        terms = down(place, e, lefts[e], rights, down_weight, down_other, parts, terms)
    arrived = lax.all_to_all(terms, TP, split_axis=0, concat_axis=0, tiled=True)
    summed = arrived.astype(F32).sum(axis=0).astype(BF16)
    out = lax.all_to_all(summed, CHIPS, split_axis=0, concat_axis=0, tiled=True)
    return jnp.transpose(out, (1, 0, 2)).reshape(out.shape[1], -1)


def solution(mesh):
    fine = Mesh(np.asarray(mesh.devices).reshape(*SHAPE.values()), tuple(SHAPE))
    in_specs = (P(SEQ, None), P(), P(), P(SEQ, TP), P(SEQ, TP), P(TP, SEQ))
    out_specs = P(SEQ + TP, None)
    return jax.shard_map(shards, mesh=fine, in_specs=in_specs, out_specs=out_specs, check_vma=False)
```
